32 devices in a mesh: gx: 4 (over y, x), gy: 4 (over z), gz: 2 (over core).
Axes of the slice: x: 2, y: 2, z: 4, core: 2. Of those that a mesh axis runs over, the one named last changes fastest.
Arguments:
- residual: float32 [2, 128, 128, 1024], P(None, 'gx', 'gy', 'gz'), may hold values from -6 to 6
- eig_x: float32 [4, 48, 48], P('gx'), may hold values from -0.875 to 0.875
- eig_y: float32 [4, 48, 48], P('gy'), may hold values from -0.875 to 0.875
- eig_z: float32 [2, 528, 528], P('gz'), may hold values from -0.25 to 0.25
- lam_x: float32 [4, 48], P('gx'), may hold values from 0.5 to 4
- lam_y: float32 [4, 48], P('gy'), may hold values from 0.5 to 4
- lam_z: float32 [2, 528], P('gz'), may hold values from 0.5 to 4
- basis_x: float32 [4, 4, 32], P('gx'), may hold values from -2.1 to 2.1
- basis_y: float32 [4, 4, 32], P('gy'), may hold values from -2.1 to 2.1
- basis_z: float32 [2, 4, 512], P('gz'), may hold values from -2.1 to 2.1
- coarse_inverse: float32 [2048, 2048], P(('gx', 'gy', 'gz')), may hold values from -0.0064086914 to 0.0064086914
Outputs:
- precond: float32 [2, 128, 128, 1024], P(None, 'gx', 'gy', 'gz')
The draws below stay inside these ranges and needn't reach their ends.
All inputs are finite; a program needn't handle non-finite values.
Results may differ from the reference program's by a relative error of at most 0.0003.
Values sent between devices are 32-bit elements; how exact they have to be, the bound alone decides.
No kernel may reach another device: no remote copies, remote signals or barrier semaphores. Data moves between devices by JAX's collectives and lax.ppermute only.
A program may use at most 128 MiB of HBM per device.

```python
import math
import jax
import jax.numpy as jnp
from jax import lax

NODES = 8
CB = 4
NV = 2
MX = 32
MY = 32
MZ = 512
KX = 48
KY = 48
KZ = 528
NX = 128
NY = 128
NZ = 1024
NC = 2048
N_GX = 4
N_GY = 4
N_GZ = 2


def block_levels(stream_key, shape, split, low, top_value):
    def one(dim, blocks):
        steps = jax.random.uniform(jax.random.fold_in(jax.random.fold_in(stream_key, 6), dim), (blocks,), jnp.float32, low / len(split), top_value / len(split))
        return jnp.repeat(jnp.exp(steps), shape[dim] // blocks).reshape((-1,) + (1,) * (len(shape) - dim - 1))

    gain = one(*split[0])
    for cut in split[1:]:
        gain = gain * one(*cut)
    return gain


def noise(own_key, extent, width, most, shards=(), kind=jnp.bfloat16):
    entries = width * jax.random.normal(own_key, extent, jnp.float32)
    if shards:
        entries = entries * block_levels(own_key, extent, shards, -0.22, 0.18)
    return jnp.clip(entries, -most, most).astype(kind)


def setup_inputs(seed: int = 0) -> dict:
    key_of = jax.random.split(jax.random.key(seed), 12)
    residual = noise(key_of[0], (NV, NX, NY, NZ), 1.0, 6.0, ((1, 4), (2, 4), (3, 2)), jnp.float32)
    eig_x = noise(key_of[1], (N_GX, KX, KX), KX ** -0.5, 0.875, ((0, 4),), jnp.float32)
    eig_y = noise(key_of[2], (N_GY, KY, KY), KY ** -0.5, 0.875, ((0, 4),), jnp.float32)
    eig_z = noise(key_of[3], (N_GZ, KZ, KZ), KZ ** -0.5, 0.25, ((0, 2),), jnp.float32)
    lam_x = jnp.clip(jnp.exp(math.log(4.0) - 2.0794415 * jax.random.uniform(key_of[4], (N_GX, KX), jnp.float32) ** block_levels(key_of[4], (N_GX, KX), ((0, 4),), -0.2, 0.2)), 0.5, 4.0)
    lam_y = jnp.clip(jnp.exp(math.log(4.0) - 2.0794415 * jax.random.uniform(key_of[5], (N_GY, KY), jnp.float32) ** block_levels(key_of[5], (N_GY, KY), ((0, 4),), -0.2, 0.2)), 0.5, 4.0)
    lam_z = jnp.clip(jnp.exp(math.log(4.0) - 2.0794415 * jax.random.uniform(key_of[6], (N_GZ, KZ), jnp.float32) ** block_levels(key_of[6], (N_GZ, KZ), ((0, 2),), -0.2, 0.2)), 0.5, 4.0)
    basis_x = noise(key_of[7], (N_GX, CB, MX), 0.35, 2.1, ((0, 4),), jnp.float32)
    basis_y = noise(key_of[8], (N_GY, CB, MY), 0.35, 2.1, ((0, 4),), jnp.float32)
    basis_z = noise(key_of[9], (N_GZ, CB, MZ), 0.35, 2.1, ((0, 2),), jnp.float32)
    coarse_inverse = noise(key_of[10], (NC, NC), (35.0 / (MX * MY * MZ * NC) ** 0.5), 0.0064086914, ((0, 32),), jnp.float32)
    return {"residual": residual, "eig_x": eig_x, "eig_y": eig_y, "eig_z": eig_z, "lam_x": lam_x, "lam_y": lam_y, "lam_z": lam_z, "basis_x": basis_x, "basis_y": basis_y, "basis_z": basis_z, "coarse_inverse": coarse_inverse}


HIGH = lax.Precision.HIGHEST


def local_solve(ext, vec_x, vec_y, vec_z, val_x, val_y, val_z):
    spec = jnp.einsum('vabc,ai->vibc', ext, vec_x, precision=HIGH)
    spec = jnp.einsum('vibc,bj->vijc', spec, vec_y, precision=HIGH)
    spec = jnp.einsum('vijc,ck->vijk', spec, vec_z, precision=HIGH)
    spec = spec / (val_x[:, None, None] + val_y[None, :, None] + val_z[None, None, :])[None]
    back = jnp.einsum('vijk,ai->vajk', spec, vec_x, precision=HIGH)
    back = jnp.einsum('vajk,bj->vabk', back, vec_y, precision=HIGH)
    back = jnp.einsum('vabk,ck->vabc', back, vec_z, precision=HIGH)
    return back


def reference(residual, eig_x, eig_y, eig_z, lam_x, lam_y, lam_z, basis_x, basis_y, basis_z, coarse_inverse):
    padded = jnp.pad(residual, ((0, 0), (NODES, NODES), (NODES, NODES), (NODES, NODES)))

    def one_brick(linear):
        brick_i = (linear // (N_GY * N_GZ)).astype(jnp.int32)
        brick_j = ((linear // N_GZ) % N_GY).astype(jnp.int32)
        brick_k = (linear % N_GZ).astype(jnp.int32)
        zero = jnp.zeros((), jnp.int32)
        ext = lax.dynamic_slice(padded, (zero, brick_i * MX, brick_j * MY, brick_k * MZ), (NV, KX, KY, KZ))
        solved = local_solve(ext, eig_x[brick_i], eig_y[brick_j], eig_z[brick_k], lam_x[brick_i], lam_y[brick_j], lam_z[brick_k])
        return solved[:, NODES:NODES + MX, NODES:NODES + MY, NODES:NODES + MZ]

    stacked = lax.map(one_brick, jnp.arange(N_GX * N_GY * N_GZ, dtype=jnp.int32))
    stacked = stacked.reshape(N_GX, N_GY, N_GZ, NV, MX, MY, MZ)
    local = jnp.transpose(stacked, (3, 0, 4, 1, 5, 2, 6)).reshape(NV, NX, NY, NZ)

    field = residual.reshape(NV, N_GX, MX, N_GY, MY, N_GZ, MZ)
    part = jnp.einsum('viajbkc,ipa->vipjbkc', field, basis_x, precision=HIGH)
    part = jnp.einsum('vipjbkc,jqb->vipjqkc', part, basis_y, precision=HIGH)
    coarse = jnp.einsum('vipjqkc,ksc->ijkpqsv', part, basis_z, precision=HIGH).reshape(NC, NV)
    coarse_sol = jnp.dot(coarse_inverse, coarse, precision=HIGH)
    blocks = coarse_sol.reshape(N_GX, N_GY, N_GZ, CB, CB, CB, NV)
    spread = jnp.einsum('ijkpqsv,ksc->ijpqvkc', blocks, basis_z, precision=HIGH)
    spread = jnp.einsum('ijpqvkc,jqb->ipvjbkc', spread, basis_y, precision=HIGH)
    spread = jnp.einsum('ipvjbkc,ipa->viajbkc', spread, basis_x, precision=HIGH).reshape(NV, NX, NY, NZ)
    return local + spread
```

```python
import functools

import jax
import jax.numpy as jnp
from jax import lax
from jax.experimental import pallas as pl
from jax.experimental.pallas import tpu as pltpu
from jax.sharding import PartitionSpec as P

F32 = jnp.float32
BF16 = jnp.bfloat16
HIGH = lax.Precision.HIGHEST
LANES = 128
SUB = 8
VMEM_BYTES = 60 * 2**20


def split(x):
    hi = x.astype(BF16)
    return hi, (x - hi.astype(F32)).astype(BF16)


def dot(a, b):
    return lax.dot_general(a, b, (((1,), (0,)), ((), ())), preferred_element_type=F32)


def dot_high(a, b, dims):
    return lax.dot_general(a, b, (dims, ((), ())), precision=HIGH, preferred_element_type=F32)


def col3(x):
    hi, lo = split(x)
    return jnp.concatenate([hi, lo, hi], axis=0)


def row3(x):
    hi, lo = split(x)
    return jnp.concatenate([hi, lo, hi], axis=1)


def onehot(rows, cols, row_of, col_of):
    r = lax.broadcasted_iota(jnp.int32, (rows, cols), 0)
    c = lax.broadcasted_iota(jnp.int32, (rows, cols), 1)
    return jnp.where(row_of(r) == col_of(c), 1.0, 0.0).astype(F32)


def same(v):
    return v


def put3(ref, x):
    hi, lo = split(x)
    n = x.shape[1]
    ref[:, 0:n] = hi
    ref[:, n : 2 * n] = hi
    ref[:, 2 * n : 3 * n] = lo


def spread_rows(ref, mat):
    rows, cols = mat.shape[0] * SUB, mat.shape[1] * SUB
    left = onehot(rows, mat.shape[0], lambda r: r // SUB, same)
    right = onehot(mat.shape[1], cols, same, lambda c: c // SUB)
    big = dot_high(left, dot_high(mat, right, ((1,), (0,))), ((1,), (0,)))
    put3(ref, big * onehot(rows, cols, lambda r: r % SUB, lambda c: c % SUB))


def prep_body(ex, ey, ez, bx, by, bz, wy, kx, wz, wyi, kxi, wzt, kxy, kxyt, bz64, *, own):
    mx, my, mz = own
    wx = (ex.shape[0] - mx) // 2
    wyid = (ey.shape[0] - my) // 2
    w = (ez.shape[0] - mz) // 2
    exv, eyv = ex[...], ey[...]
    spread_rows(kx, exv.T)
    spread_rows(kxi, exv[wx : wx + mx])
    put3(wy, eyv.T)
    put3(wyi, eyv[wyid : wyid + my])
    full = ez.shape[0]
    pad = wz.shape[1] - full
    ezv = jnp.concatenate([ez[...], jnp.zeros((full, pad), F32)], axis=1)
    mid = ezv[w : w + mz]
    mh, ml = split(mid)
    lh, ll = split(ezv[:w])
    hh, hl = split(ezv[w + mz :])
    wz[0:mz, :] = mh
    wz[mz : 2 * mz, :] = mh
    wz[2 * mz : 3 * mz, :] = ml
    f = [v.astype(F32) for v in (hh, lh, hh, ll, hl)]
    zero = jnp.zeros((LANES - 6 * w, full + pad), F32)
    wz[3 * mz :, :] = jnp.concatenate(f + [zero, lh.astype(F32)], axis=0).astype(BF16)
    th, tl = split(mid.T)
    n = full + pad
    wzt[0:n, :] = th
    wzt[n : 2 * n, :] = th
    wzt[2 * n : 3 * n, :] = tl
    cb = bx.shape[0]
    nf = cb * cb * cb
    bxv, byv = bx[...], by[...]
    rx = onehot(nf, cb, lambda r: r // (cb * cb), same)
    ry = onehot(nf, cb, lambda r: (r // cb) % cb, same)
    bx64 = dot_high(rx, bxv, ((1,), (0,)))
    by64 = dot_high(ry, byv, ((1,), (0,)))
    bz64[...] = dot_high(onehot(nf, cb, lambda r: r % cb, same), bz[...], ((1,), (0,)))
    area = mx * my
    xa = dot_high(bx64, onehot(mx, area, same, lambda c: c // my), ((1,), (0,)))
    ya = dot_high(by64, onehot(my, area, same, lambda c: c % my), ((1,), (0,)))
    put3(kxyt, xa * ya)
    xr = onehot(area, mx, lambda r: (r // SUB) % mx, same)
    yr = onehot(area, my, lambda r: (r // (SUB * mx)) * SUB + r % SUB, same)
    put3(kxy, dot_high(xr, bx64, ((1,), (1,))) * dot_high(yr, by64, ((1,), (1,))))


def restrict_body(res, kxyt, bz64, out):
    vectors = res.shape[0]
    area = res.shape[1] * res.shape[2]
    nf = bz64.shape[0]
    r = lax.broadcasted_iota(jnp.int32, (nf, out.shape[1]), 0)
    c = lax.broadcasted_iota(jnp.int32, (nf, out.shape[1]), 1)
    acc = jnp.zeros((nf, out.shape[1]), F32)
    for v in range(vectors):
        part = dot(kxyt[...], col3(res[v].reshape(area, res.shape[3])))
        col = jnp.sum(part * bz64[...], axis=1, keepdims=True)
        acc = jnp.where(c == r + v * nf, col, acc)
    out[...] = jnp.sum(acc, axis=0, keepdims=True)


def coarse_body(me, rows, inv, out, *, vectors):
    nf = inv.shape[0]
    pairs = inv.shape[1] // (2 * nf)
    low = lax.broadcasted_iota(jnp.int32, (1, 2 * nf), 1) < nf

    def step(e, accs):
        a = rows[pl.ds((2 * e) ^ me[0], 1), :]
        b = rows[pl.ds((2 * e + 1) ^ me[0], 1), :]
        m = inv[:, pl.ds(pl.multiple_of(e * 2 * nf, 2 * nf), 2 * nf)]
        both = (
            jnp.where(low, a, pltpu.roll(b, nf, 1)),
            jnp.where(low, pltpu.roll(a, nf, 1), b),
        )
        return tuple(acc + m * x for acc, x in zip(accs, both))

    zero = jnp.zeros((nf, 2 * nf), F32)
    accs = lax.fori_loop(0, pairs, step, (zero,) * vectors)
    for v in range(vectors):
        out[v] = jnp.broadcast_to(jnp.sum(accs[v], axis=1, keepdims=True), (nf, LANES))


def forward_body(pos, own, xs, xd, ylo, yhi, clo, chi, wy, kx, t_out, *rest):
    edges, ybuf = rest[:-1], rest[-1]
    w = xs.shape[0]
    mx = own.shape[1]
    wym = wy[...]

    def plane(lo, mid, hi):
        return dot(wym, col3(jnp.concatenate([lo, mid, hi], axis=0)))

    def own_step(a, _):
        ybuf[a + w] = plane(ylo[0, a], own[0, a], yhi[0, a])
        return 0

    def halo_step(a, _):
        ybuf[a + pos[0]] = plane(clo[a], xs[a], chi[a])
        ybuf[a + pos[1]] = plane(clo[a + w], xd[a], chi[a + w])
        return 0

    lax.fori_loop(0, mx, own_step, 0, unroll=4)
    lax.fori_loop(0, w, halo_step, 0, unroll=2)
    full, _, lanes = ybuf.shape

    def xstep(g, _):
        at = pl.ds(pl.multiple_of(g * SUB, SUB), SUB)
        block = ybuf[:, at, :].reshape(full * SUB, lanes)
        t_out[:, at, :] = dot(kx[...], col3(block)).reshape(full, SUB, lanes)
        return 0

    lax.fori_loop(0, ybuf.shape[1] // SUB, xstep, 0)
    for n, e in enumerate(edges):
        e[...] = t_out[:, :, pl.ds(pl.multiple_of(pos[2 + n], LANES), LANES)]


def back_body(use, t, zl, zh, wz, lx, ly, lz, wyi, kxi, wzt, kxy, sol, bz64, out, ubuf, *, width):
    full_x, full_y, lanes = t.shape
    group = SUB
    lane = lax.broadcasted_iota(jnp.int32, (group * full_y, LANES), 1)
    lzv = lz[...]
    lyv = ly[...]
    wyim = wyi[...]
    mlow = (lane >= LANES - width) & (use[0] > 0)
    mhigh = (lane < width) & (use[1] > 0)

    def zstep(g, _):
        at = pl.ds(g * group, group)
        hi, lo = split(t[at].reshape(group * full_y, lanes))
        edge = jnp.where(mhigh, zh[at].reshape(group * full_y, LANES), 0.0)
        edge = jnp.where(mlow, zl[at].reshape(group * full_y, LANES), edge)
        ehi = edge.astype(BF16).astype(F32)
        packed = ehi + pltpu.roll(edge - ehi, 2 * width, 1) + pltpu.roll(ehi, 4 * width, 1)
        spec = dot(jnp.concatenate([hi, lo, hi, packed.astype(BF16)], axis=1), wz[...])
        for k in range(group):
            p = g * group + k
            den = (lyv + lx[0, p]) + lzv
            ubuf[p] = dot(wyim, col3(spec[k * full_y : (k + 1) * full_y] / den))
        return 0

    lax.fori_loop(0, full_x // group, zstep, 0)
    mx = out.shape[0]
    rows = mx * SUB
    g3 = col3(sol[:, 0:1] * bz64[...])

    def ystep(g, _):
        at = pl.ds(pl.multiple_of(g * SUB, SUB), SUB)
        block = ubuf[:, at, :].reshape(full_x * SUB, ubuf.shape[2])
        res = dot(row3(dot(kxi[...], col3(block))), wzt[...])
        res = res + dot(kxy[pl.ds(pl.multiple_of(g * rows, rows), rows), :], g3)
        out[:, at, :] = res.reshape(mx, SUB, lanes)
        return 0

    lax.fori_loop(0, ubuf.shape[1] // SUB, ystep, 0)


def call(fn, name, args, outs, scalars=(), scratch=(), blocks=None):
    specs = [pl.BlockSpec(memory_space=pltpu.SMEM if n in scalars else pltpu.VMEM) for n in range(len(args))]
    return pl.pallas_call(
        fn,
        name=name,
        in_specs=specs,
        out_shape=outs,
        scratch_shapes=list(scratch),
        compiler_params=pltpu.CompilerParams(vmem_limit_bytes=VMEM_BYTES),
    )(*args)


def shape(*dims, dtype=F32):
    return jax.ShapeDtypeStruct(dims, dtype)


def chain(count):
    forward = [(i, i + 1) for i in range(count - 1)]
    return forward, [(b, a) for a, b in forward]


def gather_coarse(row, axes):
    buf = row
    for axis in reversed(axes):
        count = lax.axis_size(axis)
        bit = 1
        while bit < count:
            other = lax.ppermute(buf, axis, [(i, i ^ bit) for i in range(count)])
            buf = jnp.concatenate([buf, other], axis=0)
            bit *= 2
    return buf


def body(
    residual, eig_x, eig_y, eig_z, lam_x, lam_y, lam_z, basis_x, basis_y, basis_z, coarse_inverse
):
    vectors, mx, my, mz = residual.shape
    fx, fy, fz = eig_x.shape[1], eig_y.shape[1], eig_z.shape[1]
    width = (fz - mz) // 2
    pz = -(-fz // LANES) * LANES
    nf = coarse_inverse.shape[0]
    i = lax.axis_index("gx")
    k = lax.axis_index("gz")
    ngx, ngy, ngz = (lax.axis_size(a) for a in ("gx", "gy", "gz"))
    odd = i % 2

    near = [(a, a ^ 1) for a in range(ngx) if (a ^ 1) < ngx]
    far = [(a, ((a + 1) ^ 1) - 1) for a in range(ngx) if 0 <= ((a + 1) ^ 1) - 1 < ngx]
    near_edge = lax.dynamic_slice_in_dim(residual, jnp.where(odd == 0, mx - width, 0), width, 1)
    far_edge = lax.dynamic_slice_in_dim(residual, jnp.where(odd == 1, mx - width, 0), width, 1)
    relay = ngx == 4
    y_forward, y_backward = chain(ngy)
    xs, xd = [None] * vectors, [None] * vectors
    xd[0] = lax.ppermute(far_edge[0], "gx", far)
    xs[0] = lax.ppermute(near_edge[0], "gx", near)
    ylo = lax.ppermute(residual[:, :, my - width :], "gy", y_forward)
    yhi = lax.ppermute(residual[:, :, :width], "gy", y_backward)
    for v in range(1, vectors):
        if relay:
            hop = lax.ppermute(far_edge[v], "gx", [(1, 3), (2, 0)])
            xd[v] = lax.ppermute(hop, "gx", [(3, 2), (0, 1)])
        else:
            xd[v] = lax.ppermute(far_edge[v], "gx", far)
        xs[v] = lax.ppermute(near_edge[v], "gx", near)

    wy, kx, wz, wyi, kxi, wzt, kxy, kxyt, bz64 = call(
        functools.partial(prep_body, own=(mx, my, mz)),
        "prep",
        (eig_x[0], eig_y[0], eig_z[0], basis_x[0], basis_y[0], basis_z[0]),
        [
            shape(fy, 3 * fy, dtype=BF16),
            shape(fx * SUB, 3 * fx * SUB, dtype=BF16),
            shape(3 * mz + LANES, pz, dtype=BF16),
            shape(my, 3 * fy, dtype=BF16),
            shape(mx * SUB, 3 * fx * SUB, dtype=BF16),
            shape(3 * pz, mz, dtype=BF16),
            shape(mx * my, 3 * nf, dtype=BF16),
            shape(nf, 3 * mx * my, dtype=BF16),
            shape(nf, mz),
        ],
    )
    row = call(restrict_body, "restrict", (residual, kxyt, bz64), shape(1, vectors * nf))
    rows = gather_coarse(row, ("gx", "gy", "gz"))
    linear = (i * ngy + lax.axis_index("gy")) * ngz + k
    sol = call(
        functools.partial(coarse_body, vectors=vectors),
        "coarse",
        (linear.astype(jnp.int32)[None], rows, coarse_inverse),
        shape(vectors, nf, LANES),
        scalars=(0,),
    )

    high = jnp.int32(fx - width)
    first = jnp.where(odd == 0, high, 0)
    if ngz == 2:
        edge_pos = [jnp.where(k == 0, mz - LANES, 0)]
    else:
        edge_pos = [jnp.int32(mz - LANES), jnp.int32(0)]
    pos = jnp.stack([first, high - first] + edge_pos).astype(jnp.int32)
    use = jnp.stack([k > 0, k < ngz - 1]).astype(jnp.int32)
    lz = jnp.concatenate([lam_z, jnp.ones((1, pz - fz), F32)], axis=1)
    ly = lam_y.reshape(fy, 1)
    z_forward, z_backward = chain(ngz)
    pieces = []
    for v in range(vectors):
        last = jnp.concatenate([xs[v][:, my - width :], xd[v][:, my - width :]], axis=0)
        start = jnp.concatenate([xs[v][:, :width], xd[v][:, :width]], axis=0)
        clo = lax.ppermute(last, "gy", y_forward)
        chi = lax.ppermute(start, "gy", y_backward)
        t, *edges = call(
            forward_body,
            "forward",
            (pos, residual[v : v + 1], xs[v], xd[v], ylo[v : v + 1], yhi[v : v + 1], clo, chi, wy, kx),
            [shape(fx, fy, mz)] + [shape(fx, fy, LANES)] * len(edge_pos),
            scalars=(0,),
            scratch=[pltpu.VMEM((fx, fy, mz), F32)],
        )
        if ngz == 2:
            zl = zh = lax.ppermute(edges[0], "gz", [(0, 1), (1, 0)])
        else:
            zl = lax.ppermute(edges[0], "gz", z_forward)
            zh = lax.ppermute(edges[1], "gz", z_backward)
        pieces.append(
            call(
                functools.partial(back_body, width=width),
                "back",
                (use, t, zl, zh, wz, lam_x, ly, lz, wyi, kxi, wzt, kxy, sol[v], bz64),
                shape(mx, my, mz),
                scalars=(0, 5),
                scratch=[pltpu.VMEM((fx, my, pz), F32)],
            )
        )
    return jnp.stack(pieces)


def solution(mesh):
    in_specs = (
        P(None, "gx", "gy", "gz"),
        P("gx", None, None),
        P("gy", None, None),
        P("gz", None, None),
        P("gx", None),
        P("gy", None),
        P("gz", None),
        P("gx", None, None),
        P("gy", None, None),
        P("gz", None, None),
        P(("gx", "gy", "gz"), None),
    )
    out_specs = P(None, "gx", "gy", "gz")
    return jax.shard_map(body, mesh=mesh, in_specs=in_specs, out_specs=out_specs, check_vma=False)
```

```python
import functools

import jax
import jax.numpy as jnp
from jax import lax
from jax.experimental import pallas as pl
from jax.experimental.pallas import tpu as pltpu
from jax.sharding import PartitionSpec as P


F32 = jnp.float32
BF16 = jnp.bfloat16
HIGH = lax.Precision.HIGHEST
LANES = 128
SUB = 8


def split(x):
    hi = x.astype(BF16)
    return hi, (x - hi.astype(F32)).astype(BF16)


def dot(a, b):
    return lax.dot_general(a, b, (((1,), (0,)), ((), ())), preferred_element_type=F32)


def dot_high(a, b, dims):
    return lax.dot_general(a, b, (dims, ((), ())), precision=HIGH, preferred_element_type=F32)


def col3(x):
    hi, lo = split(x)
    return jnp.concatenate([hi, lo, hi], axis=0)


def row3(x):
    hi, lo = split(x)
    return jnp.concatenate([hi, lo, hi], axis=1)


def onehot(rows, cols, row_of, col_of):
    r = lax.broadcasted_iota(jnp.int32, (rows, cols), 0)
    c = lax.broadcasted_iota(jnp.int32, (rows, cols), 1)
    return jnp.where(row_of(r) == col_of(c), 1.0, 0.0).astype(F32)


def same(v):
    return v


def put3(ref, x):
    hi, lo = split(x)
    n = x.shape[1]
    ref[:, 0:n] = hi
    ref[:, n : 2 * n] = hi
    ref[:, 2 * n : 3 * n] = lo


def prep_body(ly, *refs, own, count):
    sources, outs, bufs, sems = refs[:count], refs[count : -count - 1], refs[-count - 1 : -1], refs[-1]
    copies = [pltpu.make_async_copy(s, b, sems.at[n]) for n, (s, b) in enumerate(zip(sources, bufs))]
    for c in copies:
        c.start()
    for c in copies:
        c.wait()
    prep_math(ly, *bufs, *outs, own=own)


def prep_math(
    ly, ex, ey, ez, lx, lz, bx, by, bz, wy, wx, wz, wyi, wxi, wzt, kxy, kxyt, bz64, rden, *, own
):
    mx, my, mz = own
    gx, gy = (ex.shape[0] - mx) // 2, (ey.shape[0] - my) // 2
    w = (ez.shape[0] - mz) // 2
    exv, eyv = ex[...], ey[...]
    put3(wx, exv.T)
    put3(wxi, exv[gx : gx + mx])
    put3(wy, eyv.T)
    put3(wyi, eyv[gy : gy + my])
    full = ez.shape[0]
    pad = wz.shape[1] - full
    ezv = jnp.concatenate([ez[...], jnp.zeros((full, pad), F32)], axis=1)
    mid = ezv[w : w + mz]
    mh, ml = split(mid)
    lh, ll = split(ezv[:w])
    hh, hl = split(ezv[w + mz :])
    wz[0:mz, :] = mh
    wz[mz : 2 * mz, :] = mh
    wz[2 * mz : 3 * mz, :] = ml
    f = [v.astype(F32) for v in (hh, lh, hh, ll, hl)]
    zero = jnp.zeros((LANES - 6 * w, full + pad), F32)
    wz[3 * mz :, :] = jnp.concatenate(f + [zero, lh.astype(F32)], axis=0).astype(BF16)
    th, tl = split(mid.T)
    n = full + pad
    wzt[0:n, :] = th
    wzt[n : 2 * n, :] = th
    wzt[2 * n : 3 * n, :] = tl
    cb = bx.shape[0]
    nf = cb * cb * cb
    bxv, byv = bx[...], by[...]
    rx = onehot(nf, cb, lambda r: r // (cb * cb), same)
    ry = onehot(nf, cb, lambda r: (r // cb) % cb, same)
    bx64 = dot_high(rx, bxv, ((1,), (0,)))
    by64 = dot_high(ry, byv, ((1,), (0,)))
    bz64[...] = dot_high(onehot(nf, cb, lambda r: r % cb, same), bz[...], ((1,), (0,)))
    area = mx * my
    xa = dot_high(bx64, onehot(mx, area, same, lambda c: c // my), ((1,), (0,)))
    ya = dot_high(by64, onehot(my, area, same, lambda c: c % my), ((1,), (0,)))
    put3(kxyt, xa * ya)
    xr = onehot(area, mx, lambda r: r // my, same)
    yr = onehot(area, my, lambda r: r % my, same)
    put3(kxy, dot_high(xr, bx64, ((1,), (1,))) * dot_high(yr, by64, ((1,), (1,))))
    fx = ex.shape[0]
    lxc = jnp.sum(onehot(fx, fx, same, same) * lx[...], axis=1, keepdims=True)
    lzv = jnp.concatenate([lz[...], jnp.zeros((1, pad), F32)], axis=1)
    base = lxc + lzv

    def recip_step(q, _):
        rden[q] = 1.0 / (base + ly[0, q])
        return 0

    lax.fori_loop(0, rden.shape[0], recip_step, 0)


def restrict_body(res, kxyt, bz64, out, buf, sems):
    vectors = res.shape[0]
    area = res.shape[1] * res.shape[2]
    nf = bz64.shape[0]
    copies = [pltpu.make_async_copy(res.at[v], buf.at[v], sems.at[v]) for v in range(vectors)]
    for c in copies:
        c.start()
    r = lax.broadcasted_iota(jnp.int32, (nf, out.shape[1]), 0)
    c = lax.broadcasted_iota(jnp.int32, (nf, out.shape[1]), 1)
    acc = jnp.zeros((nf, out.shape[1]), F32)
    for v in range(vectors):
        copies[v].wait()
        part = dot(kxyt[...], col3(buf[v].reshape(area, res.shape[3])))
        col = jnp.sum(part * bz64[...], axis=1, keepdims=True)
        acc = jnp.where(c == r + v * nf, col, acc)
    out[...] = jnp.sum(acc, axis=0, keepdims=True)


def coarse_body(a, b, inv, out, rows, *, vectors, bits, sizes):
    half = a.shape[0]
    rows[0:half] = a[...]
    rows[half : 2 * half] = b[...]
    me = 0
    for axis, count in sizes:
        me = me * count + lax.axis_index(axis)

    def slot(d):
        m = 0
        for n, b in enumerate(bits):
            m = m | (((d >> b) & 1) << n)
        return pl.ds(m, 1)

    nf = inv.shape[0]
    pairs = inv.shape[1] // (2 * nf)
    low = lax.broadcasted_iota(jnp.int32, (1, 2 * nf), 1) < nf

    def step(e, accs):
        even = rows[slot((2 * e) ^ me), :]
        odd = rows[slot((2 * e + 1) ^ me), :]
        m = inv[:, pl.ds(pl.multiple_of(e * 2 * nf, 2 * nf), 2 * nf)]
        both = (
            jnp.where(low, even, pltpu.roll(odd, nf, 1)),
            jnp.where(low, pltpu.roll(even, nf, 1), odd),
        )
        return tuple(acc + m * x for acc, x in zip(accs, both))

    zero = jnp.zeros((nf, 2 * nf), F32)
    accs = lax.fori_loop(0, pairs, step, (zero,) * vectors)
    for v in range(vectors):
        out[v] = jnp.broadcast_to(jnp.sum(accs[v], axis=1, keepdims=True), (nf, LANES))


def forward_body(own, xs, xd, ylo, yhi, clo, chi, wy, wx, t_out, *rest, v):
    edges, (ybuf, mine, sem) = rest[:-3], rest[-3:]
    w = xs.shape[0]
    mx = own.shape[1]
    wym = wy[...]
    high = w + mx
    near = jnp.where(lax.axis_index("gx") % 2 == 0, high, 0)
    load = pltpu.make_async_copy(own.at[v], mine, sem)
    load.start()

    def plane(lo, mid, hi):
        return dot(wym, col3(jnp.concatenate([lo, mid, hi], axis=0)))

    def own_step(a, _):
        ybuf[a + w] = plane(ylo[v, a], mine[a], yhi[v, a])
        return 0

    def halo_step(a, _):
        ybuf[a + near] = plane(clo[a], xs[a], chi[a])
        ybuf[a + high - near] = plane(clo[a + w], xd[a], chi[a + w])
        return 0

    lax.fori_loop(0, w, halo_step, 0, unroll=2)
    load.wait()
    lax.fori_loop(0, mx, own_step, 0, unroll=4)
    wxm = wx[...]

    def xstep(g, _):
        block = jnp.swapaxes(ybuf[:, pl.ds(pl.multiple_of(g * SUB, SUB), SUB), :], 0, 1)
        for k in range(SUB):
            t_out[g * SUB + k] = dot(wxm, col3(block[k]))
        return 0

    lax.fori_loop(0, ybuf.shape[1] // SUB, xstep, 0)
    last = t_out.shape[2] - LANES
    if len(edges) == 1:
        at = [pl.multiple_of(jnp.where(lax.axis_index("gz") == 0, last, 0), LANES)]
    else:
        at = [last, 0]
    for e, p in zip(edges, at):
        e[...] = t_out[:, :, pl.ds(p, LANES)]


def back_body(t, zl, zh, wz, rden, wxi, wyi, wzt, kxy, sol, bz64, *rest, width, v, group, ngz):
    out, ubuf, obuf, sems = rest[-4:]
    full_y, full_x, lanes = t.shape
    rows = group * full_x
    lane = lax.broadcasted_iota(jnp.int32, (rows, LANES), 1)
    wxim = wxi[...]
    k = lax.axis_index("gz")
    mlow = (lane >= LANES - width) & (k > 0)
    mhigh = (lane < width) & (k < ngz - 1)

    def zstep(g, _):
        at = pl.ds(g * group, group)
        hi, lo = split(t[at].reshape(rows, lanes))
        edge = jnp.where(mhigh, zh[at].reshape(rows, LANES), 0.0)
        edge = jnp.where(mlow, zl[at].reshape(rows, LANES), edge)
        ehi = edge.astype(BF16).astype(F32)
        packed = ehi + pltpu.roll(edge - ehi, 2 * width, 1) + pltpu.roll(ehi, 4 * width, 1)
        spec = dot(jnp.concatenate([hi, lo, hi, packed.astype(BF16)], axis=1), wz[...])
        for k in range(group):
            q = g * group + k
            ubuf[q] = dot(wxim, col3(spec[k * full_x : (k + 1) * full_x] * rden[q]))
        return 0

    lax.fori_loop(0, full_y // group, zstep, 0)
    wyim = wyi[...]
    my = wyim.shape[0]
    g3 = col3(sol[v, :, 0:1] * bz64[...])

    def copy(g):
        part = pl.ds(g * SUB, SUB)
        return pltpu.make_async_copy(obuf.at[part], out.at[v, part], sems.at[g])

    def ystep(g, _):
        part = pl.ds(pl.multiple_of(g * SUB, SUB), SUB)
        block = jnp.swapaxes(ubuf[:, part, :], 0, 1)
        y = [dot(wyim, col3(block[k])) for k in range(SUB)]
        at = pl.ds(pl.multiple_of(g * SUB * my, SUB * my), SUB * my)
        res = dot(row3(jnp.concatenate(y, axis=0)), wzt[...]) + dot(kxy[at, :], g3)
        obuf[part] = res.reshape(SUB, my, lanes)
        copy(g).start()
        return 0

    steps = obuf.shape[0] // SUB
    lax.fori_loop(0, steps, ystep, 0)
    for g in range(steps):
        copy(g).wait()


def join_body(a, b, out):
    out[0 : a.shape[0]] = a[...]
    out[a.shape[0] :] = b[...]


def corner_body(xs, xd, last, start):
    w, my, _ = xs.shape
    for n, x in enumerate((xs, xd)):
        last[n * w : (n + 1) * w] = x[:, my - w :, :]
        start[n * w : (n + 1) * w] = x[:, :w, :]


def call(fn, args, outs, scalars=(), scratch=(), hbm=(), anys=(), out_any=False, mib=10, **kw):
    def spec(n):
        space = pltpu.SMEM if n in scalars else pltpu.HBM if n in hbm else pl.ANY if n in anys else pltpu.VMEM
        return pl.BlockSpec(memory_space=space)

    def place(n, x):
        if n in scalars or n in anys:
            return x
        return pltpu.with_memory_space_constraint(x, pltpu.HBM if n in hbm else pltpu.VMEM)

    if out_any:
        kw["out_specs"] = pl.BlockSpec(memory_space=pl.ANY)
    return pl.pallas_call(
        fn,
        in_specs=[spec(n) for n in range(len(args))],
        out_shape=outs,
        scratch_shapes=list(scratch),
        compiler_params=pltpu.CompilerParams(vmem_limit_bytes=mib * 2**20),
        **kw,
    )(*[place(n, x) for n, x in enumerate(args)])


def shape(*dims, dtype=F32):
    return pltpu.VMEM(dims, dtype)


def chain(count):
    forward = [(i, i + 1) for i in range(count - 1)]
    return forward, [(b, a) for a, b in forward]


def coarse_steps(sizes):
    base, steps = 0, []
    for axis in ("gz", "gy", "gx"):
        bits = sizes[axis].bit_length() - 1
        steps += [(axis, 1 << b, base + b) for b in range(bits)]
        base += bits
    rank = {"gz": 0, "gy": 2, "gx": 3}
    return sorted(steps, key=lambda s: (1 if s[0] == "gx" and s[1] > 1 else rank[s[0]], s[1]))


def gather_coarse(row, steps):
    buf = row
    for n, (axis, bit, _) in enumerate(steps):
        pairs = [(i, i ^ bit) for i in range(lax.axis_size(axis))]
        other = lax.ppermute(buf, axis, pairs)
        if n == len(steps) - 1:
            return buf, other
        buf = call(join_body, (buf, other), shape(2 * buf.shape[0], buf.shape[1]), mib=1)


def body(
    residual, eig_x, eig_y, eig_z, lam_x, lam_y, lam_z, basis_x, basis_y, basis_z, coarse_inverse
):
    vectors, mx, my, mz = residual.shape
    fx, fy, fz = eig_x.shape[1], eig_y.shape[1], eig_z.shape[1]
    width = (fz - mz) // 2
    pz = -(-fz // LANES) * LANES
    nf = coarse_inverse.shape[0]
    i = lax.axis_index("gx")
    ngx, ngy, ngz = (lax.axis_size(a) for a in ("gx", "gy", "gz"))
    odd = i % 2

    near = [(a, a ^ 1) for a in range(ngx) if (a ^ 1) < ngx]
    far = [(a, ((a + 1) ^ 1) - 1) for a in range(ngx) if 0 <= ((a + 1) ^ 1) - 1 < ngx]
    near_edge = lax.dynamic_slice_in_dim(residual, jnp.where(odd == 0, mx - width, 0), width, 1)
    far_edge = lax.dynamic_slice_in_dim(residual, jnp.where(odd == 1, mx - width, 0), width, 1)
    relay = False
    y_forward, y_backward = chain(ngy)
    xs, xd = [None] * vectors, [None] * vectors
    xd[0] = lax.ppermute(far_edge[0], "gx", far)
    xs[0] = lax.ppermute(near_edge[0], "gx", near)
    ylo = lax.ppermute(residual[:, :, my - width :], "gy", y_forward)
    yhi = lax.ppermute(residual[:, :, :width], "gy", y_backward)
    for v in range(1, vectors):
        if relay:
            hop = lax.ppermute(far_edge[v], "gx", [(1, 3), (2, 0)])
            xd[v] = lax.ppermute(hop, "gx", [(3, 2), (0, 1)])
        else:
            xd[v] = lax.ppermute(far_edge[v], "gx", far)
        xs[v] = lax.ppermute(near_edge[v], "gx", near)

    prep_in = (lam_y, eig_x[0], eig_y[0], eig_z[0], lam_x, lam_z, basis_x[0], basis_y[0], basis_z[0])
    wy, wx, wz, wyi, wxi, wzt, kxy, kxyt, bz64, rden = call(
        functools.partial(prep_body, own=(mx, my, mz), count=8),
        prep_in,
        [
            shape(fy, 3 * fy, dtype=BF16),
            shape(fx, 3 * fx, dtype=BF16),
            shape(3 * mz + LANES, pz, dtype=BF16),
            shape(my, 3 * fy, dtype=BF16),
            shape(mx, 3 * fx, dtype=BF16),
            shape(3 * pz, mz, dtype=BF16),
            shape(mx * my, 3 * nf, dtype=BF16),
            shape(nf, 3 * mx * my, dtype=BF16),
            shape(nf, mz),
            shape(fy, fx, pz),
        ],
        scalars=(0,),
        hbm=range(1, 9),
        scratch=[pltpu.VMEM(a.shape, F32) for a in prep_in[1:]] + [pltpu.SemaphoreType.DMA((8,))],
        mib=20,
    )
    row = call(
        restrict_body,
        (residual, kxyt, bz64),
        shape(1, vectors * nf),
        hbm=(0,),
        scratch=[pltpu.VMEM(residual.shape, F32), pltpu.SemaphoreType.DMA((vectors,))],
        mib=16,
    )
    steps = coarse_steps({"gx": ngx, "gy": ngy, "gz": ngz})
    sol = call(
        functools.partial(
            coarse_body,
            vectors=vectors,
            bits=[s[2] for s in steps],
            sizes=(("gx", ngx), ("gy", ngy), ("gz", ngz)),
        ),
        gather_coarse(row, steps) + (coarse_inverse,),
        shape(vectors, nf, LANES),
        scratch=[pltpu.VMEM((ngx * ngy * ngz, vectors * nf), F32)],
        mib=4,
    )

    z_forward, z_backward = chain(ngz)
    group = SUB
    out = None
    for v in range(vectors):
        last, start = call(corner_body, (xs[v], xd[v]), [shape(2 * width, width, mz)] * 2, mib=1)
        clo = lax.ppermute(last, "gy", y_forward)
        chi = lax.ppermute(start, "gy", y_backward)
        t, *edges = call(
            functools.partial(forward_body, v=v),
            (residual, xs[v], xd[v], ylo, yhi, clo, chi, wy, wx),
            [shape(fy, fx, mz)] + [shape(fy, fx, LANES)] * (1 if ngz == 2 else 2),
            hbm=(0,),
            scratch=[
                pltpu.VMEM((fx, fy, mz), F32),
                pltpu.VMEM((mx, my, mz), F32),
                pltpu.SemaphoreType.DMA(()),
            ],
            mib=12,
        )
        if ngz == 2:
            zl = zh = lax.ppermute(edges[0], "gz", [(0, 1), (1, 0)])
        else:
            zl = lax.ppermute(edges[0], "gz", z_forward)
            zh = lax.ppermute(edges[1], "gz", z_backward)
        args = (t, zl, zh, wz, rden, wxi, wyi, wzt, kxy, sol, bz64)
        extra = {}
        if out is not None:
            extra["input_output_aliases"] = {len(args): 0}
            args = args + (out,)
        out = call(
            functools.partial(back_body, width=width, v=v, group=group, ngz=ngz),
            args,
            jax.ShapeDtypeStruct((vectors, mx, my, mz), F32),
            anys=(11,) if v else (),
            out_any=True,
            scratch=[
                pltpu.VMEM((fy, mx, pz), F32),
                pltpu.VMEM((mx, my, mz), F32),
                pltpu.SemaphoreType.DMA((mx // SUB,)),
            ],
            mib=14,
            **extra,
        )
    return out


def solution(mesh):
    in_specs = (
        P(None, "gx", "gy", "gz"),
        P("gx", None, None),
        P("gy", None, None),
        P("gz", None, None),
        P("gx", None),
        P("gy", None),
        P("gz", None),
        P("gx", None, None),
        P("gy", None, None),
        P("gz", None, None),
        P(("gx", "gy", "gz"), None),
    )
    out_specs = P(None, "gx", "gy", "gz")

    return jax.shard_map(body, mesh=mesh, in_specs=in_specs, out_specs=out_specs, check_vma=False)
```
